32 devices in a mesh: head: 8 (over z, x), client: 4 (over y, core).
Axes of the slice: x: 2, y: 2, z: 4, core: 2. Of those that a mesh axis runs over, the one named last changes fastest.
Arguments:
- client_ids: int32 [32], replicated, may hold values from 0 to 127, as said below
- client_table: bfloat16 [128, 256], replicated, may hold values from -6 to 6
- in_weight: bfloat16 [256, 4096], P(None, 'client'), may hold values from -0.375 to 0.375
- in_bias: float32 [4096], P('client'), may hold values from -3 to 3
- head_weight: bfloat16 [4096, 131072], P('client', 'head'), may hold values from -0.09375 to 0.09375
- tokens: int32 [32, 256], P(('head', 'client')), may hold values from 0 to 255
- labels: int32 [32, 256], P(('head', 'client')), may hold values from 0 to 255
- byte_table: bfloat16 [256, 4096], P(None, 'client'), may hold values from -5.5 to 6.7
- out_table: bfloat16 [256, 4096], P(None, 'client'), may hold values from -5.625 to 5.625
Outputs:
- head_grad: bfloat16 [4096, 131072], P('client', 'head')
- in_grad: float32 [256, 4096], P(None, 'client')
- losses: float32 [32], P(('head', 'client'))
The draws below stay inside these ranges and needn't reach their ends.
Inputs may be any that keep to these rules, and one draw needn't show every extreme that they name: `client_ids`: distinct population indices.
All inputs are finite; a program needn't handle non-finite values.
Results may differ from the reference program's by a relative error of at most 0.0085.
Values may be sent and summed in bfloat16 or wider, within the bound.
A program may use at most 128 MiB of HBM per device.

```python
import jax
import jax.numpy as jnp
from jax import lax

H = 4096
E = 256
D = 4096
VOCAB = 256
SEQ = 256
CLIENTS = 32
NPOP = 128
P_SIZE = 131072


def draw_client_ids(key, part):
    return jax.random.permutation(key, NPOP)[:CLIENTS].astype(jnp.int32)


def table_parts(key):
    noise_key = jax.random.fold_in(jax.random.fold_in(key, 7), 0)
    values = jnp.clip(jax.random.normal(noise_key, (VOCAB, D), jnp.float32), -5.5, 5.5)
    return values


def draw_byte_table(key, part):
    values = table_parts(key)
    return values.astype(jnp.bfloat16)


def draw_out_table(key, part):
    values = jnp.clip(jax.random.normal(jax.random.fold_in(key, 11), (VOCAB, D), jnp.float32), -5.5, 5.5)
    return values.astype(jnp.bfloat16)


def touch_ends(entries, key, low, largest):
    spot = [jax.random.randint(jax.random.fold_in(key, axis), (), 0, length) for axis, length in enumerate(entries.shape)]
    widest = entries.shape.index(max(entries.shape))
    next_to = spot[:widest] + [(spot[widest] + 1) % entries.shape[widest]] + spot[widest + 1:]
    return entries.at[tuple(spot)].set(low).at[tuple(next_to)].set(largest)


def level_of(stream_key, dims, pieces, low, top_value):
    level, own = 1.0, jax.random.fold_in(stream_key, 6)
    for position, shards_of in pieces:
        heights = jnp.exp(jax.random.uniform(jax.random.fold_in(own, position), (shards_of,), jnp.float32, low / len(pieces), top_value / len(pieces)))
        level = level * jnp.repeat(heights, dims[position] // shards_of).reshape([-1 if axis == position else 1 for axis in range(len(dims))])
    return level


def scatter_about(own_key, dims, scale, limit, shards=(), held_as=jnp.bfloat16):
    loudness = level_of(own_key, dims, shards, -0.22, 0.18) if shards else 1.0
    entries = jax.random.normal(own_key, dims, jnp.float32) * scale * loudness
    return jnp.minimum(jnp.maximum(entries, -limit), limit).astype(held_as)


def setup_inputs(seed: int = 0) -> dict:
    keys = jax.random.split(jax.random.key(seed), 10)
    client_ids = draw_client_ids(jax.random.fold_in(keys[9], 71), 0)
    client_table = scatter_about(keys[1], (NPOP, E), 1.0, 6.0)
    in_weight = scatter_about(keys[2], (E, H), E ** -0.5, 0.375, ((1, 4),))
    in_bias = scatter_about(keys[3], (H,), 0.5, 3.0, ((0, 4),), jnp.float32)
    head_weight = scatter_about(keys[4], (H, P_SIZE), H ** -0.5, 0.09375, ((0, 4), (1, 8)))
    tokens = touch_ends(jax.random.randint(keys[5], (CLIENTS, SEQ), 0, VOCAB), jax.random.fold_in(keys[5], 1), 0, VOCAB - 1).astype(jnp.int32)
    labels = touch_ends(jax.random.randint(keys[6], (CLIENTS, SEQ), 0, VOCAB), jax.random.fold_in(keys[6], 1), 0, VOCAB - 1).astype(jnp.int32)
    byte_table = draw_byte_table(jax.random.fold_in(keys[9], 71), 0)
    out_table = draw_out_table(jax.random.fold_in(keys[9], 71), 0)
    return dict(client_ids=client_ids, client_table=client_table, in_weight=in_weight, in_bias=in_bias, head_weight=head_weight, tokens=tokens, labels=labels, byte_table=byte_table, out_table=out_table)


EPSILON = 1e-06
learn_rate = 0.1

def client_loss(factor_a, factor_b, inputs, label_row, out_table):
    depth = factor_a.shape[0]
    rank_size = factor_a.shape[1]
    normed_in = inputs * lax.rsqrt(lax.optimization_barrier(jnp.mean(inputs * inputs, -1, keepdims=True)) + EPSILON)
    low_rank = jnp.dot(normed_in, factor_a, precision=lax.Precision.HIGHEST)
    adapted = inputs + jnp.dot(low_rank, factor_b, precision=lax.Precision.HIGHEST) / jnp.sqrt(jnp.float32(depth * rank_size))
    normed = (adapted * lax.rsqrt(lax.optimization_barrier(jnp.mean(adapted * adapted, -1, keepdims=True)) + EPSILON)).astype(jnp.bfloat16)
    logits = lax.dot_general(normed, out_table, (((1,), (1,)), ((), ())), preferred_element_type=jnp.float32)
    logits = logits * (4.0 / jnp.sqrt(jnp.float32(depth)))
    log_total = jax.nn.logsumexp(logits, -1)
    vocab_ids = lax.broadcasted_iota(jnp.int32, logits.shape, 1)
    picked = lax.optimization_barrier(jnp.sum(jnp.where(vocab_ids == label_row[:, None], logits, 0.0), -1))
    return jnp.sum(log_total - picked)

def train_client(factor_row, token_row, label_row, byte_table, out_table):
    depth = byte_table.shape[1]
    split_at = factor_row.shape[0] // 2
    rank_size = split_at // depth
    start_a = factor_row[:split_at].reshape(depth, rank_size).astype(jnp.float32)
    start_b = factor_row[split_at:].reshape(rank_size, depth).astype(jnp.float32)
    onehot = (token_row[:, None] == lax.broadcasted_iota(jnp.int32, (token_row.shape[0], byte_table.shape[0]), 1)).astype(jnp.bfloat16)
    inputs = jnp.dot(onehot, byte_table, preferred_element_type=jnp.float32)
    loss_grad = jax.value_and_grad(client_loss, argnums=(0, 1))
    first_loss, (grad_a, grad_b) = loss_grad(start_a, start_b, inputs, label_row, out_table)
    middle_a = start_a - learn_rate * grad_a
    middle_b = start_b - learn_rate * grad_b
    second_loss, (grad_a, grad_b) = loss_grad(middle_a, middle_b, inputs, label_row, out_table)
    final_a = middle_a - learn_rate * grad_a
    final_b = middle_b - learn_rate * grad_b
    deltas = jnp.concatenate([(final_a - start_a).reshape(-1), (final_b - start_b).reshape(-1)]).astype(jnp.bfloat16)
    return (deltas, first_loss / token_row.shape[0])

def reference(client_ids, client_table, in_weight, in_bias, head_weight, tokens, labels, byte_table, out_table):
    chosen = client_table[client_ids]
    preact = jnp.dot(chosen, in_weight, preferred_element_type=jnp.float32) + in_bias
    hidden = jnp.maximum(preact, 0.0).astype(jnp.bfloat16)
    factors = jnp.dot(hidden, head_weight, preferred_element_type=jnp.float32).astype(jnp.bfloat16)
    blocks = CLIENTS // 8

    def run_block(record):
        return jax.vmap(lambda fac, tok, lab: train_client(fac, tok, lab, byte_table, out_table))(record[0], record[1], record[2])
    deltas, losses = lax.map(run_block, (factors.reshape(blocks, 8, -1), tokens.reshape(blocks, 8, -1), labels.reshape(blocks, 8, -1)))
    deltas = deltas.reshape(CLIENTS, -1)
    losses = losses.reshape(CLIENTS)
    head_grad = lax.dot_general(hidden, deltas, (((0,), (0,)), ((), ())), preferred_element_type=jnp.float32).astype(jnp.bfloat16)
    hidden_back = lax.dot_general(deltas, head_weight, (((1,), (1,)), ((), ())), preferred_element_type=jnp.float32)
    masked = jnp.where(preact > 0, hidden_back, 0.0)
    in_grad = lax.dot_general(chosen.astype(jnp.float32), masked, (((0,), (0,)), ((), ())), precision=lax.Precision.HIGHEST)
    return (head_grad, in_grad, losses)
```

```python
import jax
import jax.numpy as jnp
from jax import lax
from jax.sharding import PartitionSpec as P

EPSILON = 1e-06
learn_rate = 0.1


FULL = lax.Precision.HIGHEST


def mm(x, y, over_x=1, over_y=0):
    return lax.dot_general(
        x, y, (((over_x,), (over_y,)), ((), ())), precision=FULL, preferred_element_type=jnp.float32
    )


def exact(x, y, over_x, over_y):
    return lax.dot_general(
        x, y, (((over_x,), (over_y,)), ((), ())), preferred_element_type=jnp.float32
    )


def halves(x):
    top = lax.reduce_precision(x, 8, 7)
    rest = x - top
    return jnp.concatenate([top.astype(jnp.bfloat16), rest.astype(jnp.bfloat16)], 1)


def inner_step(u, n_in, m_out, k_bb, gram_io, mean_in, pair_count, depth, scale):
    uk = mm(u, k_bb)
    z = gram_io + scale * mm(u, m_out, 1, 1)
    q = mean_in + jnp.sum(u * (2.0 * scale * n_in + (scale * scale) * uk), -1, keepdims=True) / depth
    r = lax.rsqrt(q + EPSILON)
    kappa = 4.0 / jnp.sqrt(jnp.float32(depth))
    logits = (kappa * r) * z
    top = jnp.max(logits, -1, keepdims=True)
    raised = jnp.exp(logits - top)
    total = jnp.sum(raised, -1, keepdims=True)
    row_count = jnp.sum(pair_count, -1, keepdims=True)
    loss = jnp.sum(row_count * (jnp.log(total) + top)) - jnp.sum(pair_count * logits)
    slope = row_count * (raised / total) - pair_count
    dz = (kappa * r) * slope
    dr = kappa * jnp.sum(slope * z, -1, keepdims=True)
    e = dr * (-1.0 / depth) * (r * r * r)
    gu = scale * (mm(dz, m_out) + e * (n_in + scale * uk))
    w = mm(dz, u, 0, 0)
    x = e * u
    y = mm(u, x, 0, 0)
    return loss, gu, w, x, y


def table_products(byte_full, out_full):
    depth = byte_full.shape[1]
    gram_ii = exact(byte_full, byte_full, 1, 1)
    gram_io = exact(byte_full, out_full, 1, 1)
    gram_oo = exact(out_full, out_full, 1, 1)
    size = gram_ii.shape[0]
    diagonal = lax.broadcasted_iota(jnp.int32, (size, size), 0) == lax.broadcasted_iota(
        jnp.int32, (size, size), 1
    )
    mean_in = jnp.sum(jnp.where(diagonal, gram_ii, 0.0), -1, keepdims=True) / depth
    return gram_ii, gram_io, gram_oo, mean_in


def train_client(factor_row, token_row, label_row, byte_full, out_full, products):
    gram_ii, gram_io, gram_oo, mean_in = products
    vocab, depth = byte_full.shape
    split_at = factor_row.shape[0] // 2
    rank = split_at // depth
    scale = 1.0 / jnp.sqrt(jnp.float32(depth * rank))
    a0 = factor_row[:split_at].reshape(depth, rank)
    b0 = factor_row[split_at:].reshape(rank, depth)
    ids = lax.broadcasted_iota(jnp.int32, (vocab, token_row.shape[0]), 0)
    pair_count = exact(
        (ids == token_row[None, :]).astype(jnp.bfloat16),
        (ids == label_row[None, :]).astype(jnp.bfloat16),
        1,
        1,
    )
    rn = lax.rsqrt(mean_in + EPSILON)
    u0 = rn * exact(byte_full, a0, 1, 0)
    n0 = exact(byte_full, b0, 1, 1)
    m0 = exact(out_full, b0, 1, 1)
    k0 = exact(b0, b0, 1, 1)
    fixed = (gram_io, mean_in, pair_count, depth, scale)
    first_loss, gu0, w0, x0, y0 = inner_step(u0, n0, m0, k0, *fixed)
    rate = learn_rate * scale
    w0, x0, y0 = -rate * w0, -rate * x0, (-rate * scale) * y0
    u1 = u0 - learn_rate * rn * mm(gram_ii, rn * gu0)
    n1 = n0 + mm(gram_io, w0) + mm(gram_ii, x0) + mm(n0, y0)
    m1 = m0 + mm(gram_oo, w0) + mm(gram_io, x0, 0, 0) + mm(m0, y0)
    cross = k0 + mm(y0, k0, 0, 0) + mm(w0, m0, 0, 0) + mm(x0, n0, 0, 0)
    k1 = cross + mm(cross, y0) + mm(m1, w0, 0, 0) + mm(n1, x0, 0, 0)
    _, gu1, w1, x1, y1 = inner_step(u1, n1, m1, k1, *fixed)
    w1, x1, y1 = -rate * w1, -rate * x1, (-rate * scale) * y1
    ga = (-learn_rate) * rn * (gu0 + gu1)
    wf = w0 + w1 + mm(w0, y1)
    xf = x0 + x1 + mm(x0, y1)
    yf = y0 + y1 + mm(y0, y1)
    da = exact(byte_full, halves(ga), 0, 0)
    da = da[:, :rank] + da[:, rank:]
    db = (
        exact(halves(wf), out_full, 0, 0)
        + exact(halves(xf), byte_full, 0, 0)
        + exact(halves(yf), b0, 0, 0)
    )
    db = db[:rank] + db[rank:]
    deltas = jnp.concatenate([da.astype(jnp.bfloat16).reshape(-1), db.astype(jnp.bfloat16).reshape(-1)])
    return deltas, first_loss / token_row.shape[0]


def local(
    client_ids, client_table, in_weight, in_bias, head_weight, tokens, labels, byte_table, out_table
):
    head_count = lax.axis_size("head")
    group_count = lax.axis_size("client")
    per_device = tokens.shape[0]
    byte_full, out_full = (
        lax.all_gather(byte_table, "client", axis=1, tiled=True),
        lax.all_gather(out_table, "client", axis=1, tiled=True),
    )
    products = table_products(byte_full, out_full)
    ordered = client_ids.reshape(head_count, group_count, per_device).transpose(1, 0, 2).reshape(-1)
    chosen = client_table[ordered]
    preact = jnp.dot(chosen, in_weight, preferred_element_type=jnp.float32) + in_bias
    hidden = jnp.maximum(preact, 0.0).astype(jnp.bfloat16)
    partial = jnp.dot(hidden, head_weight, preferred_element_type=jnp.float32).astype(jnp.bfloat16)
    rows, columns = partial.shape
    parts = lax.all_to_all(
        partial.reshape(group_count, rows // group_count, columns), "client", split_axis=0, concat_axis=0
    )
    summed = jnp.sum(parts.astype(jnp.float32), 0)
    owned = lax.all_to_all(
        summed.astype(jnp.bfloat16), "head", split_axis=0, concat_axis=1, tiled=True
    )
    trained = [
        train_client(owned[i], tokens[i], labels[i], byte_full, out_full, products)
        for i in range(per_device)
    ]
    deltas = jnp.stack([t[0] for t in trained])
    losses = jnp.stack([t[1] for t in trained])
    returned = lax.all_to_all(deltas, "head", split_axis=1, concat_axis=0, tiled=True)
    received = lax.all_gather(returned, "client", axis=0, tiled=True)
    back = lax.dot_general(
        received, head_weight, (((1,), (1,)), ((), ())), preferred_element_type=jnp.float32
    )
    back = lax.all_to_all(
        back.reshape(head_count, rows // head_count, back.shape[1]), "head", split_axis=0, concat_axis=0
    )
    back = jnp.sum(back, 0)
    back = lax.all_to_all(
        jnp.broadcast_to(back[None], (head_count,) + back.shape), "head", split_axis=0, concat_axis=0
    )
    hidden_back = back.reshape(rows, back.shape[2])
    grad_sum = lax.dot_general(
        hidden, received, (((0,), (0,)), ((), ())), preferred_element_type=jnp.float32
    )
    masked = jnp.where(preact > 0, hidden_back, 0.0)
    in_grad = lax.dot_general(
        chosen.astype(jnp.float32),
        masked,
        (((0,), (0,)), ((), ())),
        precision=FULL,
    )
    return (grad_sum.astype(jnp.bfloat16), in_grad, losses)


def solution(mesh):
    placed = (
        P(),
        P(),
        P(None, "client"),
        P("client"),
        P("client", "head"),
        P(("head", "client"), None),
        P(("head", "client"), None),
        P(None, "client"),
        P(None, "client"),
    )
    return jax.shard_map(
        local,
        mesh=mesh,
        in_specs=placed,
        out_specs=(P("client", "head"), P(None, "client"), P(("head", "client"))),
        check_vma=False,
    )
```
